256 devices in a mesh: rep: 2 (over core), dp: 128 (over x, y, z).
Axes of the slice: x: 4, y: 4, z: 8, core: 2. Of those that a mesh axis runs over, the one named last changes fastest.
Arguments:
- x: bfloat16 [256, 2048, 1024], P(('rep', 'dp')), parts along dimension 0
- dy: bfloat16 [256, 2048, 1024], P(('rep', 'dp')), parts along dimension 0
- wq: bfloat16 [1, 1024, 1024], P(None, 'dp')
- wk: bfloat16 [1, 1024, 1024], P(None, 'dp')
- wv: bfloat16 [1, 1024, 1024], P(None, 'dp')
- wo: bfloat16 [1, 1024, 1024], P(None, 'dp')
- w_gate: bfloat16 [1, 1024, 3072], P(None, 'dp')
- w_up: bfloat16 [1, 1024, 3072], P(None, 'dp')
- w_down: bfloat16 [1, 3072, 1024], P(None, 'dp')
Outputs:
- output 1: bfloat16 [256, 2048, 1024], P(('rep', 'dp')), parts along dimension 0
- output 2: bfloat16 [2, 1024, 1024], P('rep', 'dp'), parts along dimension 0
- output 3: bfloat16 [2, 1024, 1024], P('rep', 'dp'), parts along dimension 0
- output 4: bfloat16 [2, 1024, 1024], P('rep', 'dp'), parts along dimension 0
- output 5: bfloat16 [2, 1024, 1024], P('rep', 'dp'), parts along dimension 0
- output 6: bfloat16 [2, 1024, 3072], P('rep', 'dp'), parts along dimension 0
- output 7: bfloat16 [2, 1024, 3072], P('rep', 'dp'), parts along dimension 0
- output 8: bfloat16 [2, 3072, 1024], P('rep', 'dp'), parts along dimension 0
There are 2 independent parts. The reference program is written for one: setup_inputs(seed, part) draws one part's arguments, and reference() takes and returns one part's arrays. A program takes and returns all parts, laid end to end along the dimension named above; an argument that names none is the same for every part.
All inputs are finite; a program needn't handle non-finite values.
Results may differ from the reference program's by a relative error of at most 0.0292.
Values are sent between devices in bfloat16 or wider.
A program may use at most 768 MiB of HBM per device.

```python
import jax
import jax.numpy as jnp
from jax import lax

SEQUENCES = 128
TOKENS = 2048
D = 1024
HEADS = 8
KV_HEADS = 8
HEAD = 128
FF = 3072
LAYERS = 1
THETA = 10000
NAMES = ("wq", "wk", "wv", "wo", "w_gate", "w_up", "w_down")
SHAPES = {
    "wq": (LAYERS, D, HEADS * HEAD),
    "wk": (LAYERS, D, KV_HEADS * HEAD),
    "wv": (LAYERS, D, KV_HEADS * HEAD),
    "wo": (LAYERS, HEADS * HEAD, D),
    "w_gate": (LAYERS, D, FF),
    "w_up": (LAYERS, D, FF),
    "w_down": (LAYERS, FF, D),
}


def bump(key, n, height):
    away = (jnp.arange(n, dtype=jnp.int32) - jax.random.randint(key, (), 0, n, jnp.int32)) % n
    return jnp.where(away < n // 8, height, 1.0)


def together(key, own, strength):
    shared = jax.random.normal(key, own.shape[1:], jnp.float32)
    return (own + strength * shared) * lax.rsqrt(1 + strength * strength)


def setup_inputs(seed: int = 0, part: int = 0) -> dict:
    kx, kdy, ka, kb, kz, kf, kh, kl, *keys = jax.random.split(jax.random.key(seed), 8 + 3 * len(NAMES))
    kx, kdy, ka, kb = (jax.random.fold_in(k, part) for k in (kx, kdy, ka, kb))
    kw, km, kv = (keys[i::3] for i in range(3))
    shape = (SEQUENCES, TOKENS, D)
    much_x, much_dy = jax.random.uniform(kz, (2,), jnp.float32, 0.0, 1.0)
    loud = 2.0 ** jax.random.uniform(jax.random.fold_in(kz, 1), (), jnp.float32, -1.0, 2.0)
    layers = 2.0 ** jax.random.uniform(kl, (LAYERS, 1, 1), jnp.float32, -1.0, 1.0)
    times = {"wq": 1.0, "wk": 1.0, "wv": 2.0, "wo": layers, "w_gate": 1.0, "w_up": bump(kh, FF, 4.0), "w_down": layers}
    x = together(ka, jax.random.normal(kx, shape, jnp.float32), much_x) * bump(kf, D, 4.0)
    dy = together(kb, jax.random.normal(kdy, shape, jnp.float32), much_dy)
    drawn = {"x": x.astype(jnp.bfloat16), "dy": (loud * dy * (SEQUENCES * TOKENS) ** -0.5).astype(jnp.bfloat16)}
    for key, name in zip(kw, NAMES, strict=True):
        drawn[name] = (jax.random.normal(key, SHAPES[name], jnp.float32) * SHAPES[name][1] ** -0.5 * times[name]).astype(jnp.bfloat16)
    return drawn


def matmul(a, w):
    return jnp.dot(a, w, preferred_element_type=jnp.float32).astype(jnp.bfloat16)


def normed(h):
    wide = h.astype(jnp.float32)
    scale = lax.rsqrt(jnp.mean(wide**2, -1, keepdims=True) + 1e-6)
    return (wide * scale).astype(jnp.bfloat16)


def turned(t, theta):
    half = t.shape[-1] // 2
    angle = jnp.arange(t.shape[0], dtype=jnp.float32)[:, None] * theta ** (-jnp.arange(half, dtype=jnp.float32) / half)
    cos, sin = jnp.cos(angle)[:, None], jnp.sin(angle)[:, None]
    a, b = t[..., :half].astype(jnp.float32), t[..., half:].astype(jnp.float32)
    return jnp.concatenate([a * cos - b * sin, b * cos + a * sin], -1).astype(jnp.bfloat16)


def seen_by(q, k, v):
    tokens, kv = q.shape[0], k.shape[1]
    q = q.reshape(tokens, kv, -1, q.shape[-1])
    scores = jnp.einsum("tgsd,ugd->gstu", q.astype(jnp.float32), k.astype(jnp.float32)) * q.shape[-1] ** -0.5
    place = jnp.arange(tokens)
    weights = jax.nn.softmax(jnp.where(place[:, None] >= place, scores, -jnp.inf), -1).astype(jnp.bfloat16)
    return jnp.einsum("gstu,ugd->tgsd", weights.astype(jnp.float32), v.astype(jnp.float32)).astype(jnp.bfloat16).reshape(tokens, -1)


def layer(h, w):
    a = normed(h)
    q, k = (turned(matmul(a, w[name]).reshape(h.shape[0], -1, HEAD), THETA) for name in ("wq", "wk"))
    h = h + matmul(seen_by(q, k, matmul(a, w["wv"]).reshape(h.shape[0], -1, HEAD)), w["wo"])
    b = normed(h)
    gate = jnp.dot(b, w["w_gate"], preferred_element_type=jnp.float32)
    up = jnp.dot(b, w["w_up"], preferred_element_type=jnp.float32)
    return h + matmul((jax.nn.silu(gate) * up).astype(jnp.bfloat16), w["w_down"])


def stack(weights, h):
    return lax.scan(lambda h, w: (layer(h, w), None), h, weights)[0]


def reference(x, dy, wq, wk, wv, wo, w_gate, w_up, w_down):
    weights = dict(zip(NAMES, (wq, wk, wv, wo, w_gate, w_up, w_down), strict=True))

    def take(so_far, sequence):
        h, by_y = sequence
        _, back = jax.vjp(stack, weights, h)
        by_weights, by_h = back(by_y)
        return jax.tree.map(lambda total, term: total + term.astype(jnp.float32), so_far, by_weights), by_h

    none_yet = {name: jnp.zeros(w.shape, jnp.float32) for name, w in weights.items()}
    by_weights, by_x = lax.scan(take, none_yet, (x, dy))
    return (by_x, *(by_weights[name].astype(jnp.bfloat16) for name in NAMES))
```

```python
import math

import jax
import jax.numpy as jnp
from jax import lax
from jax.experimental import pallas as pl
from jax.experimental.pallas import tpu as pltpu
from jax.sharding import PartitionSpec as P

HIDDEN = -2e30
NEG = -1e30
LOG2E = 1.4426950408889634
VMEM = 60 * 2**20
HEAD = 128
HEADS = 8
THETA = 10000
ROWS = 512
NAMES = ("wq", "wk", "wv", "wo", "w_gate", "w_up", "w_down")
LOW, WIDE = jnp.bfloat16, jnp.float32


def _dot(a, b, ca, cb):
    return lax.dot_general(a, b, (((ca,), (cb,)), ((), ())), preferred_element_type=WIDE)


def _once(shape, index):
    return pl.BlockSpec(shape, index, pipeline_mode=pl.Buffered(1))


def _call(kernel, name, grid, ins, outs, scratch=(), flops=0, order=None):
    return pl.pallas_call(
        kernel,
        name=name,
        grid=grid,
        in_specs=[s for _, s in ins],
        out_specs=[s for _, _, s in outs],
        out_shape=[jax.ShapeDtypeStruct(s, t) for s, t, _ in outs],
        scratch_shapes=list(scratch),
        compiler_params=pltpu.CompilerParams(dimension_semantics=order or ("arbitrary",) * len(grid), vmem_limit_bytes=VMEM),
        cost_estimate=pl.CostEstimate(flops=flops, transcendentals=0, bytes_accessed=sum(a.size * 2 for a, _ in ins) + sum(math.prod(s) * 2 for s, _, _ in outs)),
    )(*[a for a, _ in ins])


def _scale(wide):
    return lax.rsqrt(jnp.mean(wide * wide, -1, keepdims=True) + 1e-6)


def _norm_back(wide, by):
    s = _scale(wide)
    return s * by - wide * (s * s * s * jnp.mean(wide * by, -1, keepdims=True))


def _turn(t, cos, sin):
    return t * cos + pltpu.roll(t, HEAD // 2, 1) * sin


def _project(x_ref, wq_ref, wk_ref, wv_ref, cos_ref, sin_ref, a_ref, q_ref, k_ref, v_ref):
    wide = x_ref[...].astype(WIDE)
    a = (wide * _scale(wide)).astype(LOW)
    a_ref[...] = a
    cos, sin = cos_ref[...], sin_ref[...]
    for w_ref, out_ref in ((wq_ref, q_ref), (wk_ref, k_ref)):
        t = _dot(a, w_ref[...], 1, 0).astype(LOW).astype(WIDE)
        for i in range(HEADS):
            here = slice(i * HEAD, (i + 1) * HEAD)
            out_ref[:, here] = _turn(t[:, here], cos, sin).astype(LOW)
    v_ref[...] = _dot(a, wv_ref[...], 1, 0).astype(LOW)


def _attend(q_ref, k_ref, v_ref, o_ref, lse_ref, top_s, mix_s):
    bq = q_ref.shape[0]
    iq = pl.program_id(0)
    e = HEAD**-0.5 * LOG2E
    top_s[...] = jnp.full(top_s.shape, NEG, WIDE)
    mix_s[...] = jnp.zeros(mix_s.shape, WIDE)
    ones = jnp.ones((8, bq), LOW)
    heads = [slice(i * HEAD, (i + 1) * HEAD) for i in range(HEADS)]

    def block(j, masked):
        here = pl.ds(pl.multiple_of(j * bq, bq), bq)
        scores = [_dot(k_ref[here, h], q_ref[:, h], 1, 1) for h in heads]
        weights, keeps = [], []
        for i, s in enumerate(scores):
            if masked:
                ok = lax.broadcasted_iota(jnp.int32, s.shape, 1) >= lax.broadcasted_iota(jnp.int32, s.shape, 0)
                s = jnp.where(ok, s, HIDDEN)
            old = top_s[i : i + 1, :]
            top = jnp.maximum(old, s.max(axis=0, keepdims=True))
            top_s[i : i + 1, :] = top
            weights.append(jnp.exp2((s - top) * e).astype(LOW))
            keeps.append(jnp.exp2((old - top) * e))
        for i, h in enumerate(heads):
            values = jnp.concatenate([v_ref[here, h].T, ones], axis=0)
            mix_s[i] = mix_s[i] * keeps[i] + _dot(values, weights[i], 1, 0)

    lax.fori_loop(0, iq, lambda j, _: block(j, False), None)
    block(iq, True)
    for i, h in enumerate(heads):
        total = mix_s[i, HEAD : HEAD + 1, :]
        o_ref[:, h] = (mix_s[i, :HEAD, :] * (1 / total)).T.astype(LOW)
        lse_ref[i : i + 1, :] = top_s[i : i + 1, :] * HEAD**-0.5 + jnp.log(total)


def _attend_back(q_ref, k_ref, v_ref, o_ref, do_ref, lse_ref, cos_ref, sin_ref, cosall_ref, sinall_ref, dq_ref, dk_ref, dv_ref, dq_s, dk_s, dv_s, delta_s):
    bq = q_ref.shape[0]
    n = q_ref.shape[1] // HEAD
    iq = pl.program_id(1)
    scale = HEAD**-0.5
    e = scale * LOG2E
    heads = [slice(i * HEAD, (i + 1) * HEAD) for i in range(n)]

    @pl.when(iq == 0)
    def _():
        dk_s[...] = jnp.zeros_like(dk_s)
        dv_s[...] = jnp.zeros_like(dv_s)

    dq_s[...] = jnp.zeros_like(dq_s)
    for i, h in enumerate(heads):
        both = do_ref[:, h].astype(WIDE) * o_ref[:, h].astype(WIDE)
        delta_s[i : i + 1, :] = both.T.sum(axis=0, keepdims=True)

    def block(j, masked):
        here = pl.ds(pl.multiple_of(j * bq, bq), bq)
        scores = [_dot(k_ref[here, h], q_ref[:, h], 1, 1) for h in heads]
        dps = [_dot(v_ref[here, h], do_ref[:, h], 1, 1) for h in heads]
        for i, h in enumerate(heads):
            p = jnp.exp2(scores[i] * e - lse_ref[0, i : i + 1, :] * LOG2E)
            if masked:
                ok = lax.broadcasted_iota(jnp.int32, p.shape, 1) >= lax.broadcasted_iota(jnp.int32, p.shape, 0)
                p = jnp.where(ok, p, 0.0)
            ds = (p * (dps[i] - delta_s[i : i + 1, :])).astype(LOW)
            dv_s[here, h] += _dot(p.astype(LOW), do_ref[:, h], 1, 0)
            dk_s[here, h] += _dot(ds, q_ref[:, h], 1, 0)
            dq_s[i] += _dot(k_ref[here, h].T, ds, 1, 0)

    lax.fori_loop(0, iq, lambda j, _: block(j, False), None)
    block(iq, True)
    cos, sin = cos_ref[...], sin_ref[...]
    for i, h in enumerate(heads):
        dq = (dq_s[i] * scale).T.astype(LOW).astype(WIDE)
        dq_ref[:, h] = _turn(dq, cos, -sin).astype(LOW)

    @pl.when(iq == pl.num_programs(1) - 1)
    def _():
        for h in heads:
            dk = (dk_s[:, h] * scale).astype(LOW).astype(WIDE)
            dk_ref[:, h] = _turn(dk, cosall_ref[...], -sinall_ref[...]).astype(LOW)
        dv_ref[...] = dv_s[...].astype(LOW)


def _middle(x_ref, o_ref, dy_ref, wo_ref, wg_ref, wu_ref, wd_ref, b_ref, act_ref, dgate_ref, dup_ref, dh_ref, do_ref, *, chunk):
    h = (x_ref[...].astype(WIDE) + _dot(o_ref[...], wo_ref[...], 1, 0).astype(LOW).astype(WIDE)).astype(LOW)
    wide = h.astype(WIDE)
    b = (wide * _scale(wide)).astype(LOW)
    b_ref[...] = b
    dy = dy_ref[...]
    by = jnp.zeros(wide.shape, WIDE)
    for at in range(0, wg_ref.shape[1], chunk):
        here = slice(at, at + chunk)
        gate, up = _dot(b, wg_ref[:, here], 1, 0), _dot(b, wu_ref[:, here], 1, 0)
        dact = _dot(dy, wd_ref[here, :], 1, 1).astype(LOW).astype(WIDE)
        sig = jax.nn.sigmoid(gate)
        silu = gate * sig
        act_ref[:, here] = (silu * up).astype(LOW)
        dup = (dact * silu).astype(LOW)
        dgate = (dact * up * (sig + silu * (1 - sig))).astype(LOW)
        dup_ref[:, here], dgate_ref[:, here] = dup, dgate
        by += _dot(dgate, wg_ref[:, here], 1, 1) + _dot(dup, wu_ref[:, here], 1, 1)
    dh = (dy.astype(WIDE) + _norm_back(wide, by.astype(LOW).astype(WIDE)).astype(LOW).astype(WIDE)).astype(LOW)
    dh_ref[...] = dh
    do_ref[...] = _dot(dh, wo_ref[...], 1, 1).astype(LOW)


def _outer(*refs):
    n = (len(refs) - 1) // 2
    for b_ref, out_ref in zip(refs[1 : 1 + n], refs[1 + n :]):
        out_ref[...] = _dot(refs[0][...], b_ref[...], 0, 0).astype(LOW)


def _first(x_ref, dh_ref, dq_ref, dk_ref, dv_ref, wq_ref, wk_ref, wv_ref, dx_ref):
    by = _dot(dq_ref[...], wq_ref[...], 1, 1) + _dot(dk_ref[...], wk_ref[...], 1, 1) + _dot(dv_ref[...], wv_ref[...], 1, 1)
    wide = x_ref[...].astype(WIDE)
    dx_ref[...] = (dh_ref[...].astype(WIDE) + _norm_back(wide, by.astype(LOW).astype(WIDE)).astype(LOW).astype(WIDE)).astype(LOW)


def tables(tokens):
    half = HEAD // 2
    angle = jnp.arange(tokens, dtype=WIDE)[:, None] * THETA ** (-jnp.arange(half, dtype=WIDE) / half)
    cos, sin = jnp.cos(angle), jnp.sin(angle)
    return jnp.concatenate([cos, cos], 1), jnp.concatenate([-sin, sin], 1)


def project(x, att, cos, sin):
    t, d = x.shape
    rows = pl.BlockSpec((ROWS, d), lambda i: (i, 0))
    w = lambda n: _once((d, d), lambda i: (0, n))
    turn = pl.BlockSpec((ROWS, HEAD), lambda i: (i, 0))
    return _call(_project, "project", (t // ROWS,), [(x, rows), (att, w(0)), (att, w(1)), (att, w(2)), (cos, turn), (sin, turn)],
                 [((t, d), LOW, rows)] * 4, flops=6 * t * d * d)


def attend(q, k, v):
    t, d = q.shape
    rows, whole = pl.BlockSpec((ROWS, d), lambda i: (i, 0)), _once((t, d), lambda i: (0, 0))
    return _call(_attend, "attend", (t // ROWS,), [(q, rows), (k, whole), (v, whole)],
                 [((t, d), LOW, rows), ((HEADS, t), WIDE, pl.BlockSpec((HEADS, ROWS), lambda i: (0, i)))],
                 [pltpu.VMEM((HEADS, ROWS), WIDE), pltpu.VMEM((HEADS, HEAD + 8, ROWS), WIDE)], flops=2 * t * t * d)


def attend_back(q, k, v, o, do, lse, cos, sin, n=4):
    t, d = q.shape
    w = n * HEAD
    rows, whole = pl.BlockSpec((ROWS, w), lambda g, i: (i, g)), pl.BlockSpec((t, w), lambda g, i: (0, g))
    lse = lse.reshape(HEADS // n, n, t)
    turn, turns = pl.BlockSpec((ROWS, HEAD), lambda g, i: (i, 0)), _once((t, HEAD), lambda g, i: (0, 0))
    return _call(_attend_back, "attend_back", (HEADS // n, t // ROWS),
                 [(q, rows), (k, whole), (v, whole), (o, rows), (do, rows), (lse, pl.BlockSpec((1, n, ROWS), lambda g, i: (g, 0, i))),
                  (cos, turn), (sin, turn), (cos, turns), (sin, turns)],
                 [((t, d), LOW, rows), ((t, d), LOW, whole), ((t, d), LOW, whole)],
                 [pltpu.VMEM((n, HEAD, ROWS), WIDE), pltpu.VMEM((t, w), WIDE), pltpu.VMEM((t, w), WIDE), pltpu.VMEM((n, ROWS), WIDE)], flops=5 * t * t * d)


def middle(x, o, dy, att, ff, down, rows_=256, chunk=512):
    t, d = x.shape
    f = down.shape[0]
    rows, broad = pl.BlockSpec((rows_, d), lambda i: (i, 0)), pl.BlockSpec((rows_, f), lambda i: (i, 0))
    ins = [(x, rows), (o, rows), (dy, rows), (att, _once((d, d), lambda i: (0, 3))), (ff, _once((d, f), lambda i: (0, 0))), (ff, _once((d, f), lambda i: (0, 1))),
           (down, _once((f, d), lambda i: (0, 0)))]
    body = lambda *refs: _middle(*refs, chunk=chunk)
    return _call(body, "middle", (t // rows_,), ins,
                 [((t, d), LOW, rows), ((t, f), LOW, broad), ((t, f), LOW, broad), ((t, f), LOW, broad), ((t, d), LOW, rows), ((t, d), LOW, rows)],
                 flops=2 * t * d * (5 * f + 2 * d))


def outer(name, a, bs, rows=256):
    t, m = a.shape
    ins = [(a, pl.BlockSpec((t, rows), lambda i: (0, i)))] + [(b, _once(b.shape, lambda i: (0, 0))) for b in bs]
    outs = [((m, b.shape[1]), LOW, pl.BlockSpec((rows, b.shape[1]), lambda i: (i, 0))) for b in bs]
    return _call(_outer, name, (m // rows,), ins, outs, flops=2 * t * m * sum(b.shape[1] for b in bs))


def first(x, dh, dq, dk, dv, att):
    t, d = x.shape
    rows = pl.BlockSpec((ROWS, d), lambda i: (i, 0))
    w = lambda n: _once((d, d), lambda i: (0, n))
    return _call(_first, "first", (t // ROWS,), [(x, rows), (dh, rows), (dq, rows), (dk, rows), (dv, rows), (att, w(0)), (att, w(1)), (att, w(2))],
                 [((t, d), LOW, rows)], flops=6 * t * d * d)[0]


def gray(p):
    return p ^ (p >> 1)


def place(g):
    p = g
    while g := g >> 1:
        p ^= g
    return p


def flipped(sizes, axis, bit):
    def to(i):
        at = [i // (sizes[1] * sizes[2]), i // sizes[2] % sizes[1], i % sizes[2]]
        at[axis] = place(gray(at[axis]) ^ (1 << bit))
        return (at[0] * sizes[1] + at[1]) * sizes[2] + at[2]

    return [(i, to(i)) for i in range(math.prod(sizes))]


def plan(sizes, axes, bits):
    steps = []
    for axis in axes:
        codes = [gray(p) for p in range(sizes[axis])]
        for bit in bits[axis]:
            sides = [[codes.index(c) for c in sorted((c for c in codes if c >> bit & 1 == side), key=lambda c: c & ~(1 << bit))] for side in (0, 1)]
            steps.append((axis, bit, *sides))
            codes = sorted({c & ~(1 << bit) for c in codes})
    return steps


COLOURS = [((0, 1), ((0, 1), (0, 1))), ((1, 0), ((0, 1), (0, 1))), ((0, 1), ((1, 0), (1, 0))), ((1, 0), ((1, 0), (1, 0)))]


def _sides(step, j, one):
    _, _, low, high = step
    return low[j] + one * (high[j] - low[j]), high[j] + one * (low[j] - high[j])


def _split(bit_ref, *refs, steps, pieces, n):
    ins, outs = refs[:n], refs[n:]
    for colour, step in enumerate(steps):
        one = bit_ref[colour]
        for j in range(len(step[2])):
            for side, out in zip(_sides(step, j, one), (outs[2 * colour + 1], outs[2 * colour])):
                for other in range(ins[0].shape[1 - step[0]]):
                    src, dst = ((side, other), (j, other)) if step[0] == 0 else ((other, side), (other, j))
                    for which, part, start, to, width in pieces[colour]:
                        at = (*src, 0) if part is None else (*src, 0, part)
                        out[(*dst, 0, slice(None), slice(to, to + width))] = ins[which][(*at, slice(None), slice(start, start + width))]


def _sum(a, b):
    return (a.astype(WIDE) + b.astype(WIDE)).astype(LOW)


def _add_split(bit_ref, *refs, steps):
    n = len(steps)
    keeps, gots, outs = refs[:n], refs[n : 2 * n], refs[2 * n :]
    for colour, step in enumerate(steps):
        one = bit_ref[colour]
        keep, got = keeps[colour], gots[colour]
        for j in range(len(step[2])):
            for side, out in zip(_sides(step, j, one), (outs[2 * colour + 1], outs[2 * colour])):
                for other in range(keep.shape[1 - step[0]]):
                    src, dst = ((side, other), (j, other)) if step[0] == 0 else ((other, side), (other, j))
                    for z in range(keep.shape[2]):
                        out[(*dst, z)] = _sum(keep[(*src, z)], got[(*src, z)])


def _merge(bit_ref, *refs, step, n):
    keeps, gots, (send, stay) = refs[:n], refs[n : 2 * n], refs[2 * n :]
    for j in range(len(step[2])):
        for side, out in zip(_sides(step, j, bit_ref[0]), (stay, send)):
            at = 0
            for keep, got in zip(keeps, gots):
                w = keep.shape[-1]
                out[j, :, at : at + w] = _sum(keep[0, 0, side], got[0, 0, side])
                at += w


def _along(bit_ref, keep, got, send, stay, *, step):
    for j in range(len(step[2])):
        for side, out in zip(_sides(step, j, bit_ref[0]), (stay, send)):
            out[j] = _sum(keep[side], got[side])


def _finish(keep, got, *outs, pieces):
    for out, part, start, width in pieces:
        here = slice(start, start + width)
        got_here = _sum(keep[0, :, here], got[0, :, here])
        if part is None:
            outs[out][...] = got_here
        else:
            outs[out][part] = got_here


BITS = pl.BlockSpec(memory_space=pltpu.SMEM)


def _whole(a):
    return pl.BlockSpec(a.shape if hasattr(a, "shape") else a, lambda *_: (0,) * len(a.shape if hasattr(a, "shape") else a))


class Halving:
    def __init__(self, name, terms, sizes):
        self.name, self.sizes = name, sizes
        me = lax.axis_index("dp")
        at = (me // (sizes[1] * sizes[2]), me // sizes[2] % sizes[1], me % sizes[2])
        self.codes = [jnp.bitwise_xor(p, p >> 1) for p in at]
        self.plans = [plan(sizes, axes, bits) for axes, bits in COLOURS]
        self.z = plan(sizes, (2,), {2: (0, 1, 2)})
        self.columns = [(i, part if parts > 1 else None, m.shape[1]) for i, (m, parts) in enumerate(terms) for part in range(parts)]
        self.parts = [parts for _, parts in terms]
        total = sum(w for _, _, w in self.columns)
        self.width = total // len(COLOURS)
        pieces = cut(self.columns, self.width)
        blocks = [m.reshape(*sizes, *((parts,) if parts > 1 else ()), 8, m.shape[1]) for m, parts in terms]
        ins = [(self.bits(0), BITS)] + [(b, pl.BlockSpec((*sizes[:2], 1, *b.shape[3:]), lambda z, n=b.ndim: (0, 0, z) + (0,) * (n - 3))) for b in blocks]
        outs = []
        for p in self.plans:
            s = self.halved((*sizes, 8, self.width), p[0][0])
            outs += [(s, LOW, pl.BlockSpec((*s[:2], 1, *s[3:]), lambda z: (0, 0, z, 0, 0)))] * 2
        steps = [p[0] for p in self.plans]
        body = lambda *refs: _split(*refs, steps=steps, pieces=pieces, n=len(blocks))
        self.take(_call(body, f"{name}_split", (sizes[2],), ins, outs, flops=sum(m.size for m, _ in terms)), 0)

    def bits(self, n):
        return jnp.stack([self.codes[p[n][0]] >> p[n][1] & 1 for p in self.plans])

    def halved(self, s, axis):
        return tuple(d // 2 if i == axis else d for i, d in enumerate(s))

    def take(self, out, n):
        self.send, self.keep, self.n = list(out[0::2]), list(out[1::2]), n

    def exchange(self):
        steps = [p[self.n] for p in self.plans] if self.n < 4 else [self.z[self.n - 4]]
        self.got = [lax.ppermute(s, "dp", flipped(self.sizes, step[0], step[1])) for s, step in zip(self.send, steps)]

    def next(self):
        n = self.n + 1
        if n < 4:
            steps = [p[n] for p in self.plans]
            zs = 2
            spec = lambda s: pl.BlockSpec((*s[:2], zs, *s[3:]), lambda z: (0, 0, z, 0, 0))
            ins = [(self.bits(n), BITS)] + [(a, spec(a.shape)) for a in (*self.keep, *self.got)]
            outs = []
            for a, step in zip(self.keep, steps):
                s = self.halved(a.shape, step[0])
                outs += [(s, LOW, spec(s))] * 2
            body, grid = (lambda *refs: _add_split(*refs, steps=steps)), (self.sizes[2] // zs,)
        else:
            step = self.z[n - 4]
            bit = (self.codes[2] >> step[1] & 1)[None]
            ins = [(bit, BITS)] + [(a, _whole(a)) for a in (*self.keep, *self.got)]
            s = (len(step[2]), 8, self.width * len(COLOURS))
            outs = [(s, LOW, _whole(s))] * 2
            count = len(self.keep)
            body = (lambda *refs: _merge(*refs, step=step, n=count)) if n == 4 else (lambda *refs: _along(*refs, step=step))
            grid = (1,)
        self.take(_call(body, f"{self.name}_{n}", grid, ins, outs, flops=sum(a.size for a in self.keep)), n)

    def result(self):
        (keep,), (got,) = self.keep, self.got
        outs, pieces, at = [], [], 0
        for i, part, w in self.columns:
            pieces.append((i, part, at, w))
            at += w
            if not part:
                s = (8, w) if part is None else (self.parts[i], 8, w)
                outs.append((s, LOW, _whole(s)))
        got = _call(lambda *refs: _finish(*refs, pieces=pieces), f"{self.name}_sum", (1,), [(keep, _whole(keep)), (got, _whole(got))], outs, flops=keep.size)
        return [g.reshape(-1, g.shape[-1]) for g in got]


def _join_z(bit_ref, mine, got, *outs, step):
    for j in range(len(step[2])):
        for side, src in zip(_sides(step, j, bit_ref[0]), (mine, got)):
            if len(outs) == 1:
                outs[0][side] = src[j]
            else:
                for colour, out in enumerate(outs):
                    w = out.shape[-1]
                    out[0, 0, side] = src[j, :, colour * w : (colour + 1) * w]


def _join(bit_ref, *refs, steps, pieces=None):
    n = len(steps)
    mines, gots, outs = refs[:n], refs[n : 2 * n], refs[2 * n :]
    for colour, step in enumerate(steps):
        one = bit_ref[colour]
        for j in range(len(step[2])):
            for side, src in zip(_sides(step, j, one), (mines[colour], gots[colour])):
                for other in range(src.shape[1 - step[0]]):
                    at, dst = ((j, other), (side, other)) if step[0] == 0 else ((other, j), (other, side))
                    for z in range(src.shape[2]):
                        if pieces is None:
                            outs[colour][(*dst, z)] = src[(*at, z)]
                        else:
                            for which, part, start, to, width in pieces[colour]:
                                place_ = (*dst, z) if part is None else (*dst, z, part)
                                outs[which][(*place_, slice(None), slice(start, start + width))] = src[(*at, z, slice(None), slice(to, to + width))]


def cut(columns, width):
    pieces, at = [[] for _ in COLOURS], 0
    for i, part, w in columns:
        start = 0
        while start < w:
            colour, to = divmod(at, width)
            n = min(w - start, width - to)
            pieces[colour].append((i, part, start, to, n))
            start, at = start + n, at + n
    return pieces


class Doubling:
    def __init__(self, name, block, results, sizes):
        self.name, self.sizes = name, sizes
        me = lax.axis_index("dp")
        at = (me // (sizes[1] * sizes[2]), me // sizes[2] % sizes[1], me % sizes[2])
        self.codes = [jnp.bitwise_xor(p, p >> 1) for p in at]
        z = plan(sizes, (2,), {2: (0, 1, 2)})
        plans = [plan(sizes, axes, bits) for axes, bits in COLOURS]
        self.steps = [[s] for s in reversed(z)] + [list(s) for s in zip(*(reversed(p) for p in plans))]
        self.results = results
        self.held, self.n, self.width = [block[None]], 0, block.shape[1] // len(COLOURS)

    def exchange(self):
        self.got = [lax.ppermute(a, "dp", flipped(self.sizes, step[0], step[1])) for a, step in zip(self.held, self.steps[self.n])]

    def next(self):
        steps, n = self.steps[self.n], self.n
        bits = jnp.stack([self.codes[s[0]] >> s[1] & 1 for s in steps])
        nx, ny, nz = self.sizes
        body = lambda *refs: _join_z(*refs, step=steps[0])
        grid, spec, outs = (1,), _whole, None
        if n < 2:
            s = self.held[0].shape
            s = (2 * s[0], *s[1:])
            outs = [(s, LOW, _whole(s))]
        elif n == 2:
            s = (1, 1, nz, 8, self.width)
            outs = [(s, LOW, _whole(s))] * len(COLOURS)
        else:
            zs = 2 if n < 6 else 1
            grid = (nz // zs,)
            spec = lambda a: pl.BlockSpec((*a.shape[:2], zs, *a.shape[3:]), lambda z, k=len(a.shape): (0, 0, z) + (0,) * (k - 3))
            if n < 6:
                shapes = [tuple(d * 2 if i == step[0] else d for i, d in enumerate(a.shape)) for a, step in zip(self.held, steps)]
                pieces = None
            else:
                shapes = [(nx, ny, nz, *((parts,) if parts > 1 else ()), 8, w) for w, parts in self.results]
                pieces = cut([(i, part if parts > 1 else None, w) for i, (w, parts) in enumerate(self.results) for part in range(parts)], self.width)
            outs = [(s, LOW, spec(jax.ShapeDtypeStruct(s, LOW))) for s in shapes]
            body = lambda *refs: _join(*refs, steps=steps, pieces=pieces)
        ins = [(bits, BITS)] + [(a, spec(a)) for a in (*self.held, *self.got)]
        self.held, self.n = list(_call(body, f"{self.name}_{n}", grid, ins, outs, flops=sum(a.size for a in self.held))), n + 1
        if n == 6:
            return [a.reshape(-1, w) for a, (w, _) in zip(self.held, self.results)]


def gathers(w, sizes):
    d, f, rows = w["wo"].shape[1], w["w_gate"].shape[1], w["wq"].shape[0]
    parts = f // d
    down = w["w_down"].reshape(parts, rows, d).transpose(1, 0, 2).reshape(rows, f)
    att = Doubling("get_att", jnp.concatenate([w[n] for n in NAMES[:4]], 1), [(4 * d, 1)], sizes)
    return att, Doubling("get_ff", jnp.concatenate([w["w_gate"], w["w_up"], down], 1), [(2 * f, 1), (d, parts)], sizes)


def together(*groups):
    flat = lax.optimization_barrier([a for g in groups for a in g])
    out, at = [], 0
    for g in groups:
        out.append(flat[at : at + len(g)])
        at += len(g)
    return out


def local(x, dy, att, ff, down=None, summing=None):
    cos, sin = tables(x.shape[0])
    if summing is None:
        a, q, k, v = project(x, att, cos, sin)
        o, lse = attend(q, k, v)
    else:
        get_att, get_ff = att, ff
        for n in range(7):
            get_att.exchange()
            if n >= 2:
                get_ff.exchange()
            got = get_att.next()
            if n >= 2:
                get_ff.next()
        get_ff.held, got = together(get_ff.held, got)
        get_ff.exchange()
        att = got[0]
        (a, q, k, v), get_ff.got = together(project(x, att, cos, sin), get_ff.got)
        get_ff.next()
        get_ff.held, (q, k, v) = together(get_ff.held, [q, k, v])
        get_ff.exchange()
        (o, lse), get_ff.got = together(attend(q, k, v), get_ff.got)
        ff, down = get_ff.next()
    b, act, dgate, dup, dh, do = middle(x, o, dy, att, ff, down)
    (by_down,), (by_gate,), (by_up,), (by_wo,) = outer("by_down", act, [dy]), outer("by_gate", b, [dgate]), outer("by_up", b, [dup]), outer("by_wo", o, [dh])
    if summing is None:
        dq, dk, dv = attend_back(q, k, v, o, do, lse, cos, sin)
        return first(x, dh, dq, dk, dv, att), *outer("by_qkv", a, [dq, dk, dv]), by_wo, by_gate, by_up, by_down
    wide = summing("ff", [(by_gate, 1), (by_up, 1), (by_down, down.shape[0] // down.shape[1]), (by_wo, 1)])
    wide.send, (do,) = together(wide.send, [do])
    wide.exchange()
    (dq, dk, dv), wide.got = together(attend_back(q, k, v, o, do, lse, cos, sin), wide.got)
    wide.next()
    wide.send, (dq, dk, dv) = together(wide.send, [dq, dk, dv])
    wide.exchange()
    by_qkv, wide.got = together(outer("by_qkv", a, [dq, dk, dv]), wide.got)
    narrow = summing("qkv", [(g, 1) for g in by_qkv])
    narrow.exchange()
    wide.next()
    wide.send, narrow.send, (dh,) = together(wide.send, narrow.send, [dh])
    wide.exchange()
    (dx,), wide.got, narrow.got = together([first(x, dh, dq, dk, dv, att)], wide.got, narrow.got)
    for n in range(6):
        narrow.next()
        narrow.exchange()
        if n < 4:
            wide.next()
            wide.exchange()
    by_wide, by_narrow = wide.result(), narrow.result()
    return dx, *by_narrow, by_wide[3], *by_wide[:2], by_wide[2]


def solution(mesh):
    sizes = (4, 4, 8)

    def step(x, dy, *weights):
        att, ff = gathers({name: t[0] for name, t in zip(NAMES, weights, strict=True)}, sizes)
        return tuple(g[None] for g in local(x[0], dy[0], att, ff, summing=lambda name, terms: Halving(name, terms, sizes)))

    states, cut = P(("rep", "dp"), None, None), P(None, "dp", None)
    return jax.shard_map(
        step,
        mesh=mesh,
        in_specs=(states, states) + (cut,) * 7,
        out_specs=(states,) + (P("rep", "dp", None),) * 7,
        check_vma=False,
    )
```
